32 devices in a mesh: data: 32 (over z, y, x, core).
Axes of the slice: x: 2, y: 2, z: 4, core: 2. Of those that a mesh axis runs over, the one named last changes fastest.
Arguments:
- feat_img: bfloat16 [32768, 768], P('data')
- feat_txt: bfloat16 [32768, 512], P('data')
- w_img: bfloat16 [768, 512], replicated
- w_txt: bfloat16 [512, 512], replicated
- log_temp: float32 [], replicated
- logit_bias: float32 [], replicated
- pair_ids: int32 [32768], P('data')
Outputs:
- output 1: float32 [], replicated
- output 2: float32 [], replicated
- output 3: float32 [], replicated
- output 4: float32 [768, 512], replicated
- output 5: float32 [512, 512], replicated
All inputs are finite; a program needn't handle non-finite values.
Results may differ from the reference program's by a relative error of at most 0.001.
Values are sent between devices in bfloat16 or wider.
A program may use at most 1 GiB of HBM per device.

```python
import jax
import jax.numpy as jnp
from jax import lax

ROWS_DEV = 1024
DEVICES = 32
EMBED = 512
FEAT_IMG = 768
FEAT_TXT = 512
LATENT = 16

BATCH = ROWS_DEV * DEVICES


def feature_draw(base_key, feat_width):
    key_list = jax.random.split(base_key, 4)
    latents = jax.random.normal(key_list[0], (BATCH, LATENT), jnp.float32)
    basis_rows = jax.random.normal(key_list[1], (LATENT, feat_width), jnp.float32)
    center = jax.random.normal(key_list[2], (feat_width,), jnp.float32)
    noise_rows = jax.random.normal(key_list[3], (BATCH, feat_width), jnp.float32)
    feat_out = center + jnp.dot(latents, basis_rows) * LATENT ** -0.5 + 0.5 * noise_rows
    return feat_out.astype(jnp.bfloat16)


def setup_inputs(seed: int = 0) -> dict:
    key_list = jax.random.split(jax.random.key(seed), 7)
    w_img = jax.random.normal(key_list[2], (FEAT_IMG, EMBED), jnp.float32) * FEAT_IMG ** -0.5
    w_txt = jax.random.normal(key_list[3], (FEAT_TXT, EMBED), jnp.float32) * FEAT_TXT ** -0.5
    log_temp = jnp.log(10.0) + jax.random.uniform(key_list[4], (), jnp.float32, -0.5, 0.5)
    logit_bias = -jnp.log(float(BATCH)) + jax.random.uniform(key_list[5], (), jnp.float32, -0.5, 1.5)
    pair_ids = (jax.random.permutation(key_list[6], BATCH) // 2).astype(jnp.int32)
    return {
        "feat_img": feature_draw(key_list[0], FEAT_IMG),
        "feat_txt": feature_draw(key_list[1], FEAT_TXT),
        "w_img": w_img.astype(jnp.bfloat16),
        "w_txt": w_txt.astype(jnp.bfloat16),
        "log_temp": log_temp.astype(jnp.float32),
        "logit_bias": logit_bias.astype(jnp.float32),
        "pair_ids": pair_ids,
    }


def reference(feat_img, feat_txt, w_img, w_txt, log_temp, logit_bias, pair_ids):
    temp_scale = jnp.exp(log_temp)
    raw_img = jnp.dot(feat_img, w_img, preferred_element_type=jnp.float32)
    raw_txt = jnp.dot(feat_txt, w_txt, preferred_element_type=jnp.float32)
    inv_img = lax.rsqrt(jnp.sum(raw_img * raw_img, axis=1, keepdims=True))
    inv_txt = lax.rsqrt(jnp.sum(raw_txt * raw_txt, axis=1, keepdims=True))
    unit_img = raw_img * inv_img
    unit_txt = raw_txt * inv_txt
    emb_img = unit_img.astype(jnp.bfloat16)
    emb_txt = unit_txt.astype(jnp.bfloat16)

    def row_block(loop_state, block_in):
        acc_txt, loss_sum, temp_sum, bias_sum = loop_state
        emb_blk, ids_blk = block_in
        sim_tile = jnp.dot(emb_blk, emb_txt.T, preferred_element_type=jnp.float32)
        label_sign = jnp.where(ids_blk[:, None] == pair_ids[None, :], 1.0, -1.0).astype(jnp.float32)
        margin = -label_sign * (temp_scale * sim_tile + logit_bias)
        grad_tile = -label_sign * jax.nn.sigmoid(margin) / BATCH
        grad_bf = grad_tile.astype(jnp.bfloat16)
        grad_blk = jnp.dot(grad_bf, emb_txt, preferred_element_type=jnp.float32)
        acc_txt = acc_txt + jnp.dot(grad_bf.T, emb_blk, preferred_element_type=jnp.float32)
        new_state = (
            acc_txt,
            loss_sum + jnp.sum(jax.nn.softplus(margin)),
            temp_sum + jnp.sum(grad_tile * sim_tile),
            bias_sum + jnp.sum(grad_tile),
        )
        return new_state, grad_blk

    zero_sum = jnp.zeros((), jnp.float32)
    init_state = (jnp.zeros((BATCH, EMBED), jnp.float32), zero_sum, zero_sum, zero_sum)
    block_in = (emb_img.reshape(DEVICES, ROWS_DEV, EMBED), pair_ids.reshape(DEVICES, ROWS_DEV))
    final_state, grad_blocks = lax.scan(row_block, init_state, block_in)
    acc_txt, loss_sum, temp_sum, bias_sum = final_state
    grad_img = temp_scale * grad_blocks.reshape(BATCH, EMBED)
    grad_txt = temp_scale * acc_txt
    raw_grad_img = inv_img * (grad_img - unit_img * jnp.sum(unit_img * grad_img, axis=1, keepdims=True))
    raw_grad_txt = inv_txt * (grad_txt - unit_txt * jnp.sum(unit_txt * grad_txt, axis=1, keepdims=True))
    grad_w_img = jnp.dot(feat_img.T, raw_grad_img.astype(jnp.bfloat16), preferred_element_type=jnp.float32)
    grad_w_txt = jnp.dot(feat_txt.T, raw_grad_txt.astype(jnp.bfloat16), preferred_element_type=jnp.float32)
    return loss_sum / BATCH, temp_scale * temp_sum, bias_sum, grad_w_img, grad_w_txt
```

```python
import jax
import jax.numpy as jnp
from jax import lax
from jax.experimental import pallas as pl
from jax.experimental.pallas import tpu as pltpu
from jax.sharding import Mesh, PartitionSpec as P

CONTRACT_ROWS = (((0,), (0,)), ((), ()))
LOG2E = 1.4426950408889634
LN2 = 0.6931471805599453
ROWS_TILE = 512
COLS_TILE = 1024
COLS_SUB = 256
LANES = 128


def pair_patch(sim, ids_img, ids_txt, scale2, bias2):
    sign = jnp.where(ids_img == ids_txt, -1.0, 1.0)
    return (sim * scale2 + bias2) * sign, sign


def pair_kernel(n_rows, n_steps, scal_ref, img_ref, img_t_ref, txt_ref, txt_t_ref, idi_ref, idt_ref,
                dimg_ref, dtxt_ref, sums_ref, grad_even, grad_odd):
    step = pl.program_id(0)
    prev = jnp.maximum(step - 1, 0)

    @pl.when(step == 0)
    def _():
        grad_odd[...] = jnp.zeros_like(grad_odd)
        dimg_ref[...] = jnp.zeros_like(dimg_ref)
        sums_ref[...] = jnp.zeros_like(sums_ref)

    @pl.when(lax.rem(prev, n_rows) == 0)
    def _():
        dtxt_ref[...] = jnp.zeros_like(dtxt_ref)

    row_now = pl.multiple_of(lax.rem(jnp.minimum(step, n_steps - 1), n_rows) * ROWS_TILE, ROWS_TILE)
    row_prev = pl.multiple_of(lax.rem(prev, n_rows) * ROWS_TILE, ROWS_TILE)
    scale2 = scal_ref[0]
    bias2 = scal_ref[1]
    n_sub = COLS_TILE // COLS_SUB
    per_sub = COLS_SUB // LANES

    def similarity(sub):
        return jnp.dot(img_ref[pl.ds(row_now, ROWS_TILE), :], txt_t_ref[:, sub * COLS_SUB:(sub + 1) * COLS_SUB],
                       preferred_element_type=jnp.float32)

    def again(grad_now):
        def rows_again(piece, _):
            base = pl.multiple_of(row_now + piece * 64, 64)
            rows = pl.ds(pl.multiple_of(piece * 64, 64), 64)
            for block in range(COLS_TILE // LANES):
                cols = slice(block * LANES, block * LANES + LANES)
                sim = jnp.dot(img_ref[pl.ds(base, 64), :], txt_t_ref[:, cols], preferred_element_type=jnp.float32)
                margin, sign = pair_patch(sim, idi_ref[pl.ds(base, 64), :], idt_ref[0:1, cols], scale2, bias2)
                tail = jnp.exp2(-jnp.abs(margin))
                denom = 1.0 + tail
                grad = jnp.where(margin >= 0.0, 1.0, tail) * (1.0 / denom) * sign
                loss = LN2 * jnp.maximum(margin, 0.0) + jnp.log1p(tail)
                for index, term in enumerate((loss, grad * sim, grad)):
                    sums_ref[index] += jnp.sum(term.reshape(8, 8, LANES), axis=0)
                grad_now[block, rows, :] = grad.astype(jnp.bfloat16)
            return 0

        lax.fori_loop(0, ROWS_TILE // 64, rows_again, 0)

    def tile_pair(grad_now, grad_prev):
        zero = jnp.zeros((8, LANES), jnp.float32)
        sum_log, sum_gs, sum_g, sum_top = zero, zero, zero, zero
        sim_next = similarity(0)
        for sub in range(n_sub):
            cols = slice(sub * COLS_SUB, (sub + 1) * COLS_SUB)
            sim_sub = sim_next
            if sub + 1 < n_sub:
                sim_next = similarity(sub + 1)
            old = jnp.concatenate([grad_prev[sub * per_sub + k] for k in range(per_sub)], axis=1)
            dtxt_ref[:, cols] += jnp.dot(
                img_t_ref[:, pl.ds(row_prev, ROWS_TILE)], old, preferred_element_type=jnp.float32)
            piece = ROWS_TILE // n_sub
            old = jnp.concatenate(
                [grad_prev[k, sub * piece:(sub + 1) * piece, :] for k in range(COLS_TILE // LANES)], axis=1)
            dimg_ref[pl.ds(row_prev + sub * piece, piece), :] += jnp.dot(
                old, txt_ref[...], preferred_element_type=jnp.float32)
            for row in range(0, ROWS_TILE, 16):
                for lane in range(per_sub):
                    lane0 = lane * LANES
                    idt = idt_ref[:, sub * COLS_SUB + lane0:sub * COLS_SUB + lane0 + LANES]
                    pair = []
                    for line in (row, row + 8):
                        sim = sim_sub[line:line + 8, lane0:lane0 + LANES]
                        margin, sign = pair_patch(sim, idi_ref[pl.ds(row_now + line, 8), :], idt, scale2, bias2)
                        growth = jnp.exp2(margin)
                        denom = 1.0 + growth
                        grad = growth * (1.0 / denom) * sign
                        sum_gs = sum_gs + grad * sim
                        sum_g = sum_g + grad
                        if row % 64 == 0 and line == row:
                            if lane == 0:
                                chains = [None] * per_sub
                            chains[lane] = growth
                        else:
                            chains[lane] = growth + chains[lane] * denom
                        pair.append(grad)
                    grad_now[sub * per_sub + lane, row:row + 16, :] = jnp.concatenate(pair, axis=0).astype(jnp.bfloat16)
                if row % 64 == 48:
                    for prod in chains:
                        sum_log = sum_log + jnp.log1p(prod)
                        sum_top = sum_top + prod

        live = step < n_steps
        fits = jnp.sum(sum_top) < 1e30

        @pl.when(jnp.logical_and(live, fits))
        def _():
            sums_ref[0] += sum_log
            sums_ref[1] += sum_gs
            sums_ref[2] += sum_g

        @pl.when(jnp.logical_and(live, jnp.logical_not(fits)))
        def _():
            again(grad_now)

    @pl.when(lax.rem(step, 2) == 0)
    def _():
        tile_pair(grad_even, grad_odd)

    @pl.when(lax.rem(step, 2) == 1)
    def _():
        tile_pair(grad_odd, grad_even)


def pair_call(scal, img, img_t, txt, txt_t, idi, idt):
    n_img, width = img.shape
    n_txt = txt.shape[0]
    n_rows = n_img // ROWS_TILE
    n_cols = n_txt // COLS_TILE
    n_steps = n_rows * n_cols
    once = pl.Buffered(1)

    def col_now(step):
        return jnp.minimum(step, n_steps - 1) // n_rows

    def col_prev(step):
        return jnp.maximum(step - 1, 0) // n_rows

    return pl.pallas_call(
        lambda *refs: pair_kernel(n_rows, n_steps, *refs),
        grid=(n_steps + 1,),
        in_specs=[
            pl.BlockSpec(memory_space=pltpu.SMEM),
            pl.BlockSpec((n_img, width), lambda s: (0, 0), pipeline_mode=once),
            pl.BlockSpec((width, n_img), lambda s: (0, 0), pipeline_mode=once),
            pl.BlockSpec((COLS_TILE, width), lambda s: (col_prev(s), 0)),
            pl.BlockSpec((width, COLS_TILE), lambda s: (0, col_now(s))),
            pl.BlockSpec((n_img, LANES), lambda s: (0, 0), pipeline_mode=once),
            pl.BlockSpec((8, COLS_TILE), lambda s: (0, col_now(s))),
        ],
        out_specs=[
            pl.BlockSpec((n_img, width), lambda s: (0, 0)),
            pl.BlockSpec((width, COLS_TILE), lambda s: (0, col_prev(s))),
            pl.BlockSpec((3, 8, LANES), lambda s: (0, 0, 0)),
        ],
        out_shape=[
            jax.ShapeDtypeStruct((n_img, width), jnp.float32),
            jax.ShapeDtypeStruct((width, n_txt), jnp.float32),
            jax.ShapeDtypeStruct((3, 8, LANES), jnp.float32),
        ],
        scratch_shapes=[pltpu.VMEM((COLS_TILE // LANES, ROWS_TILE, LANES), jnp.bfloat16)] * 2,
        compiler_params=pltpu.CompilerParams(
            dimension_semantics=("arbitrary",), vmem_limit_bytes=60 * 1024 * 1024),
        cost_estimate=pl.CostEstimate(
            flops=6 * n_img * n_txt * width, bytes_accessed=4 * (n_img + n_txt) * width * 2,
            transcendentals=2 * n_img * n_txt),
        name="pair_tiles",
    )(scal, img, img_t, txt, txt_t, idi, idt)


def embed_rows(feat_rows, weights):
    raw_emb = jnp.dot(feat_rows, weights, preferred_element_type=jnp.float32)
    inv_norm = lax.rsqrt(jnp.sum(raw_emb * raw_emb, axis=1, keepdims=True))
    unit_emb = raw_emb * inv_norm
    return unit_emb, inv_norm, unit_emb.astype(jnp.bfloat16)


def weight_grad(feat_rows, unit_emb, inv_norm, grad_emb):
    raw_grad = inv_norm * (grad_emb - unit_emb * jnp.sum(unit_emb * grad_emb, axis=1, keepdims=True))
    high = lax.reduce_precision(raw_grad, 8, 7)
    low = (raw_grad - high).astype(jnp.bfloat16)
    out = lax.dot_general(feat_rows, high.astype(jnp.bfloat16), CONTRACT_ROWS, preferred_element_type=jnp.float32)
    return out + lax.dot_general(feat_rows, low, CONTRACT_ROWS, preferred_element_type=jnp.float32)


def solution(mesh):
    n_dev = mesh.shape["data"]
    n_z = 4
    n_p = n_dev // n_z
    grid_mesh = Mesh(mesh.devices.reshape(n_z, n_p), ("z", "p"))
    rows = P(("z", "p"))

    def local_fn(feat_img, feat_txt, w_img, w_txt, log_temp, logit_bias, pair_ids):
        total_rows = feat_img.shape[0] * n_dev
        temp_scale = jnp.exp(log_temp)
        ids_all = lax.all_gather(pair_ids, ("z", "p"), tiled=True).reshape(n_z, n_p, -1)
        ids_img = lax.dynamic_index_in_dim(ids_all, lax.axis_index("p"), 1, keepdims=False).reshape(-1)
        ids_txt = lax.dynamic_index_in_dim(ids_all, lax.axis_index("z"), 0, keepdims=False).reshape(-1)
        feat_img = lax.all_gather(feat_img, "z", tiled=True)
        feat_txt = lax.all_gather(feat_txt, "p", tiled=True)
        unit_img, inv_img, emb_img = embed_rows(feat_img, w_img)
        unit_txt, inv_txt, emb_txt = embed_rows(feat_txt, w_txt)
        scal = jnp.stack([temp_scale * LOG2E, logit_bias * LOG2E])
        idi = jnp.broadcast_to(ids_img[:, None], (ids_img.shape[0], LANES))
        idt = jnp.broadcast_to(ids_txt[None, :], (8, ids_txt.shape[0]))
        part_img, part_txt_t, sums = pair_call(scal, emb_img, emb_img.T, emb_txt, emb_txt.T, idi, idt)
        step_scale = temp_scale / total_rows
        dw_img = weight_grad(feat_img, unit_img, inv_img, step_scale * part_img)
        dw_txt = weight_grad(feat_txt, unit_txt, inv_txt, step_scale * part_txt_t.T)
        sums = jnp.sum(sums, axis=(1, 2)) / total_rows
        sums, dw_img, dw_txt = lax.psum((sums, dw_img, dw_txt), ("z", "p"))
        return sums[0], temp_scale * sums[1], sums[2], dw_img, dw_txt

    return jax.shard_map(
        local_fn,
        mesh=grid_mesh,
        in_specs=(P(("z", "p"), None), P(("z", "p"), None), P(None, None), P(None, None), P(), P(), rows),
        out_specs=(P(), P(), P(), P(None, None), P(None, None)),
        check_vma=False,
    )
```

```python
import jax
import jax.numpy as jnp
from jax import lax
from jax.experimental import pallas as pl
from jax.experimental.pallas import tpu as pltpu
from jax.sharding import Mesh, PartitionSpec as P

CONTRACT_ROWS = (((0,), (0,)), ((), ()))
LOG2E = 1.4426950408889634
LN2 = 0.6931471805599453
ROWS_TILE = 1024
COLS_TILE = 512
COLS_SUB = 256
LANES = 128


def pair_patch(sim, ids_img, ids_txt, scale2, bias2):
    sign = jnp.where(ids_img == ids_txt, -1.0, 1.0)
    return (sim * scale2 + bias2) * sign, sign


def pair_kernel(n_rows, n_steps, scal_ref, img_ref, img_t_ref, txt_ref, txt_t_ref, idi_ref, idt_ref,
                dimg_ref, dtxt_ref, sums_ref, grad_even, grad_odd):
    step = pl.program_id(0)
    prev = jnp.maximum(step - 1, 0)

    @pl.when(step == 0)
    def _():
        grad_odd[...] = jnp.zeros_like(grad_odd)
        dimg_ref[...] = jnp.zeros_like(dimg_ref)
        sums_ref[...] = jnp.zeros_like(sums_ref)

    @pl.when(lax.rem(prev, n_rows) == 0)
    def _():
        dtxt_ref[...] = jnp.zeros_like(dtxt_ref)

    row_now = pl.multiple_of(lax.rem(jnp.minimum(step, n_steps - 1), n_rows) * ROWS_TILE, ROWS_TILE)
    row_prev = pl.multiple_of(lax.rem(prev, n_rows) * ROWS_TILE, ROWS_TILE)
    scale2 = scal_ref[0]
    bias2 = scal_ref[1]
    n_sub = COLS_TILE // COLS_SUB
    per_sub = COLS_SUB // LANES

    def similarity(sub):
        return jnp.dot(img_ref[pl.ds(row_now, ROWS_TILE), :], txt_t_ref[:, sub * COLS_SUB:(sub + 1) * COLS_SUB],
                       preferred_element_type=jnp.float32)

    def again(grad_now):
        def rows_again(piece, _):
            base = pl.multiple_of(row_now + piece * 64, 64)
            rows = pl.ds(pl.multiple_of(piece * 64, 64), 64)
            for block in range(COLS_TILE // LANES):
                cols = slice(block * LANES, block * LANES + LANES)
                sim = jnp.dot(img_ref[pl.ds(base, 64), :], txt_t_ref[:, cols], preferred_element_type=jnp.float32)
                margin, sign = pair_patch(sim, idi_ref[pl.ds(base, 64), :], idt_ref[0:1, cols], scale2, bias2)
                tail = jnp.exp2(-jnp.abs(margin))
                denom = 1.0 + tail
                grad = jnp.where(margin >= 0.0, 1.0, tail) * (1.0 / denom) * sign
                loss = LN2 * jnp.maximum(margin, 0.0) + jnp.log1p(tail)
                for index, term in enumerate((loss, grad * sim, grad)):
                    sums_ref[index] += jnp.sum(term.reshape(8, 8, LANES), axis=0)
                grad_now[block, rows, :] = grad.astype(jnp.bfloat16)
            return 0

        lax.fori_loop(0, ROWS_TILE // 64, rows_again, 0)

    def tile_pair(grad_now, grad_prev):
        zero = jnp.zeros((8, LANES), jnp.float32)
        sum_log, sum_gs, sum_g, sum_top = zero, zero, zero, zero
        sim_next = similarity(0)
        for sub in range(n_sub):
            cols = slice(sub * COLS_SUB, (sub + 1) * COLS_SUB)
            sim_sub = sim_next
            old = jnp.concatenate([grad_prev[sub * per_sub + k] for k in range(per_sub)], axis=1)
            dtxt_ref[:, cols] += jnp.dot(
                img_t_ref[:, pl.ds(row_prev, ROWS_TILE)], old, preferred_element_type=jnp.float32)
            piece = ROWS_TILE // n_sub
            old = jnp.concatenate(
                [grad_prev[k, sub * piece:(sub + 1) * piece, :] for k in range(COLS_TILE // LANES)], axis=1)
            dimg_ref[pl.ds(row_prev + sub * piece, piece), :] += jnp.dot(
                old, txt_ref[...], preferred_element_type=jnp.float32)
            if sub + 1 < n_sub:
                sim_next = similarity(sub + 1)
            for row in range(0, ROWS_TILE, 16):
                for lane in range(per_sub):
                    lane0 = lane * LANES
                    idt = idt_ref[:, sub * COLS_SUB + lane0:sub * COLS_SUB + lane0 + LANES]
                    pair = []
                    for line in (row, row + 8):
                        sim = sim_sub[line:line + 8, lane0:lane0 + LANES]
                        margin, sign = pair_patch(sim, idi_ref[pl.ds(row_now + line, 8), :], idt, scale2, bias2)
                        growth = jnp.exp2(margin)
                        denom = 1.0 + growth
                        grad = growth * (1.0 / denom) * sign
                        sum_gs = sum_gs + grad * sim
                        sum_g = sum_g + grad
                        if row % 64 == 0 and line == row:
                            if lane == 0:
                                chains = [None] * per_sub
                            chains[lane] = growth
                        else:
                            chains[lane] = growth + chains[lane] * denom
                        pair.append(grad)
                    grad_now[sub * per_sub + lane, row:row + 16, :] = jnp.concatenate(pair, axis=0).astype(jnp.bfloat16)
                if row % 64 == 48:
                    for prod in chains:
                        sum_log = sum_log + jnp.log1p(prod)
                        sum_top = sum_top + prod

        live = step < n_steps
        fits = jnp.sum(sum_top) < 1e30

        @pl.when(jnp.logical_and(live, fits))
        def _():
            sums_ref[0] += sum_log
            sums_ref[1] += sum_gs
            sums_ref[2] += sum_g

        @pl.when(jnp.logical_and(live, jnp.logical_not(fits)))
        def _():
            again(grad_now)

    @pl.when(lax.rem(step, 2) == 0)
    def _():
        tile_pair(grad_even, grad_odd)

    @pl.when(lax.rem(step, 2) == 1)
    def _():
        tile_pair(grad_odd, grad_even)


def pair_call(scal, img, img_t, txt, txt_t, idi, idt):
    n_img, width = img.shape
    n_txt = txt.shape[0]
    n_rows = n_img // ROWS_TILE
    n_cols = n_txt // COLS_TILE
    n_steps = n_rows * n_cols
    once = pl.Buffered(1)

    def col_now(step):
        return jnp.minimum(step, n_steps - 1) // n_rows

    def col_prev(step):
        return jnp.maximum(step - 1, 0) // n_rows

    return pl.pallas_call(
        lambda *refs: pair_kernel(n_rows, n_steps, *refs),
        grid=(n_steps + 1,),
        in_specs=[
            pl.BlockSpec(memory_space=pltpu.SMEM),
            pl.BlockSpec((n_img, width), lambda s: (0, 0), pipeline_mode=once),
            pl.BlockSpec((width, n_img), lambda s: (0, 0), pipeline_mode=once),
            pl.BlockSpec((COLS_TILE, width), lambda s: (col_prev(s), 0)),
            pl.BlockSpec((width, COLS_TILE), lambda s: (0, col_now(s))),
            pl.BlockSpec((n_img, LANES), lambda s: (0, 0), pipeline_mode=once),
            pl.BlockSpec((8, COLS_TILE), lambda s: (0, col_now(s))),
        ],
        out_specs=[
            pl.BlockSpec((n_img, width), lambda s: (0, 0)),
            pl.BlockSpec((width, COLS_TILE), lambda s: (0, col_prev(s))),
            pl.BlockSpec((3, 8, LANES), lambda s: (0, 0, 0)),
        ],
        out_shape=[
            jax.ShapeDtypeStruct((n_img, width), jnp.float32),
            jax.ShapeDtypeStruct((width, n_txt), jnp.float32),
            jax.ShapeDtypeStruct((3, 8, LANES), jnp.float32),
        ],
        scratch_shapes=[pltpu.VMEM((COLS_TILE // LANES, ROWS_TILE, LANES), jnp.bfloat16)] * 2,
        compiler_params=pltpu.CompilerParams(
            dimension_semantics=("arbitrary",), vmem_limit_bytes=60 * 1024 * 1024),
        cost_estimate=pl.CostEstimate(
            flops=6 * n_img * n_txt * width, bytes_accessed=4 * (n_img + n_txt) * width * 2,
            transcendentals=2 * n_img * n_txt),
        name="pair_tiles",
    )(scal, img, img_t, txt, txt_t, idi, idt)


def prep_kernel(wide, n_alias, x_ref, w_ref, *refs):
    emb_ref, emb_t_ref, raw_ref, x_out = refs[n_alias:]
    x = x_ref[...]
    x_out[...] = x
    raw = jnp.dot(x, w_ref[...], preferred_element_type=jnp.float32)
    unit = raw * lax.rsqrt(jnp.sum(raw * raw, axis=1, keepdims=True))
    emb_ref[...] = unit.astype(jnp.bfloat16)
    emb_t_ref[...] = unit.T.astype(jnp.bfloat16)
    raw_ref[...] = raw.T if wide else raw


def prep_block(x, w, index, n_blocks, bufs, wide):
    n_blk, feat = x.shape
    width = w.shape[1]
    tile = 256
    per = n_blk // tile
    n_all = n_blk * n_blocks
    rows = pl.BlockSpec((tile, width), lambda i: (index * per + i, 0))
    cols = pl.BlockSpec((width, tile), lambda i: (0, index * per + i))
    fixed = pl.BlockSpec(w.shape, lambda i: (0, 0))
    bufs = () if bufs is None else tuple(bufs)
    return pl.pallas_call(
        lambda *refs: prep_kernel(wide, len(bufs), *refs),
        grid=(per,),
        in_specs=[pl.BlockSpec((tile, feat), lambda i: (i, 0)), fixed]
        + [pl.BlockSpec(memory_space=pl.ANY)] * len(bufs),
        out_specs=[rows, cols, cols if wide else rows, pl.BlockSpec((tile, feat), lambda i: (index * per + i, 0))],
        out_shape=[
            jax.ShapeDtypeStruct((n_all, width), jnp.bfloat16),
            jax.ShapeDtypeStruct((width, n_all), jnp.bfloat16),
            jax.ShapeDtypeStruct((width, n_all) if wide else (n_all, width), jnp.float32),
            jax.ShapeDtypeStruct((n_all, feat), jnp.bfloat16),
        ],
        input_output_aliases={2 + k: k for k in range(len(bufs))},
        compiler_params=pltpu.CompilerParams(dimension_semantics=("arbitrary",), vmem_limit_bytes=60 * 1024 * 1024),
        cost_estimate=pl.CostEstimate(
            flops=2 * n_blk * feat * width, bytes_accessed=n_blk * (4 * feat + 8 * width), transcendentals=n_blk),
        name="prep_rows",
    )(x, w, *bufs)


def norm_back(raw, grad, axis):
    inv_norm = lax.rsqrt(jnp.sum(raw * raw, axis=axis, keepdims=True))
    unit = raw * inv_norm
    raw_grad = inv_norm * (grad - unit * jnp.sum(unit * grad, axis=axis, keepdims=True))
    high = raw_grad.astype(jnp.bfloat16)
    low = (raw_grad - high.astype(jnp.float32)).astype(jnp.bfloat16)
    return high, low


def tail_rows_kernel(n_steps, grad_ref, raw_ref, x_ref, out_ref, acc_ref):
    step = pl.program_id(0)

    @pl.when(step == 0)
    def _():
        acc_ref[...] = jnp.zeros_like(acc_ref)

    pieces = norm_back(raw_ref[...], grad_ref[...], 1)
    acc_ref[...] += lax.dot_general(
        x_ref[...], jnp.concatenate(pieces, axis=1), CONTRACT_ROWS, preferred_element_type=jnp.float32)

    @pl.when(step == n_steps - 1)
    def _():
        width = out_ref.shape[1]
        out_ref[...] = acc_ref[:, :width] + acc_ref[:, width:]


def tail_cols_kernel(n_steps, grad_ref, raw_ref, x_ref, out_ref, acc_ref):
    step = pl.program_id(0)

    @pl.when(step == 0)
    def _():
        acc_ref[...] = jnp.zeros_like(acc_ref)

    pieces = norm_back(raw_ref[...], grad_ref[...], 0)
    acc_ref[...] += jnp.dot(jnp.concatenate(pieces, axis=0), x_ref[...], preferred_element_type=jnp.float32)

    @pl.when(step == n_steps - 1)
    def _():
        width = out_ref.shape[1]
        out_ref[...] = (acc_ref[:width, :] + acc_ref[width:, :]).T


def tail_call(grad, raw, x, wide):
    n_all, feat = x.shape
    width = grad.shape[0] if wide else grad.shape[1]
    tile = 512
    n_steps = n_all // tile
    shape = (feat, width)
    block = pl.BlockSpec((width, tile), lambda i: (0, i)) if wide else pl.BlockSpec((tile, width), lambda i: (i, 0))
    body = tail_cols_kernel if wide else tail_rows_kernel
    return pl.pallas_call(
        lambda *refs: body(n_steps, *refs),
        grid=(n_steps,),
        in_specs=[block, block, pl.BlockSpec((tile, feat), lambda i: (i, 0))],
        out_specs=pl.BlockSpec(shape, lambda i: (0, 0)),
        out_shape=jax.ShapeDtypeStruct(shape, jnp.float32),
        scratch_shapes=[pltpu.VMEM((2 * width, feat) if wide else (feat, 2 * width), jnp.float32)],
        compiler_params=pltpu.CompilerParams(dimension_semantics=("arbitrary",), vmem_limit_bytes=60 * 1024 * 1024),
        cost_estimate=pl.CostEstimate(
            flops=4 * n_all * feat * width, bytes_accessed=n_all * (2 * feat + 8 * width), transcendentals=n_all),
        name="tail_cols" if wide else "tail_rows",
    )(grad, raw, x)


def weight_grad(feat_rows, raw_emb, grad_emb):
    inv_norm = lax.rsqrt(jnp.sum(raw_emb * raw_emb, axis=1, keepdims=True))
    unit_emb = raw_emb * inv_norm
    raw_grad = inv_norm * (grad_emb - unit_emb * jnp.sum(unit_emb * grad_emb, axis=1, keepdims=True))
    high = lax.reduce_precision(raw_grad, 8, 7)
    low = (raw_grad - high).astype(jnp.bfloat16)
    out = lax.dot_general(feat_rows, high.astype(jnp.bfloat16), CONTRACT_ROWS, preferred_element_type=jnp.float32)
    return out + lax.dot_general(feat_rows, low, CONTRACT_ROWS, preferred_element_type=jnp.float32)


def solution(mesh):
    n_dev = mesh.shape["data"]
    n_z = 4
    n_p = n_dev // n_z
    grid_mesh = Mesh(mesh.devices.reshape(n_z, n_p), ("z", "p"))

    def rotate(value, hop):
        return lax.ppermute(value, "z", [(src, (src + hop) % n_z) for src in range(n_z)])

    def swap(value, mask):
        return lax.ppermute(value, "p", [(src, src ^ mask) for src in range(n_p)])

    def local_fn(feat_img, feat_txt, w_img, w_txt, log_temp, logit_bias, pair_ids):
        total_rows = feat_img.shape[0] * n_dev
        temp_scale = jnp.exp(log_temp)
        txt_blocks = [feat_txt] + [rotate(feat_txt, hop) for hop in (1, 3, 2)]
        img_blocks = []
        for mask in range(0, n_p, 2):
            same_core = feat_img if mask == 0 else swap(feat_img, mask)
            img_blocks += [same_core, swap(same_core, 1)]

        ids_all = lax.all_gather(pair_ids, ("z", "p"), tiled=True).reshape(n_z, n_p, -1)
        my_z, my_p = lax.axis_index("z"), lax.axis_index("p")
        ids_txt = jnp.concatenate(
            [lax.dynamic_slice(ids_all, (lax.rem(my_z + n_z - hop, n_z), my_p, 0), (1, 1, ids_all.shape[2]))[0, 0]
             for hop in (0, 1, 3, 2)])
        ids_img = jnp.concatenate(
            [lax.dynamic_slice(ids_all, (my_z, jnp.bitwise_xor(my_p, mask), 0), (1, 1, ids_all.shape[2]))[0, 0]
             for mask in range(n_p)])
        id_rows = jnp.broadcast_to(ids_txt[:, None], (ids_txt.shape[0], LANES))
        id_cols = jnp.broadcast_to(ids_img[None, :], (8, ids_img.shape[0]))

        txt_all = None
        for index, block in enumerate(txt_blocks):
            txt_all = prep_block(block, w_txt, index, n_z, txt_all, False)
        img_all = None
        for index, block in enumerate(img_blocks):
            img_all = prep_block(block, w_img, index, n_p, img_all, True)
        emb_txt, emb_txt_t, raw_txt, x_txt = txt_all
        emb_img, emb_img_t, raw_img_t, x_img = img_all
        scal = jnp.stack([temp_scale * LOG2E, logit_bias * LOG2E])
        part_txt, part_img_t, sums = pair_call(scal, emb_txt, emb_txt_t, emb_img, emb_img_t, id_rows, id_cols)
        dw_txt = weight_grad(x_txt, raw_txt, part_txt)
        dw_img = weight_grad(x_img, raw_img_t.T, part_img_t.T)
        sums = jnp.sum(sums, axis=(1, 2)) / total_rows
        sums, dw_img, dw_txt = lax.psum((sums, dw_img, dw_txt), ("z", "p"))
        scale = temp_scale / total_rows
        return sums[0], temp_scale * sums[1], sums[2], scale * dw_img, scale * dw_txt

    return jax.shard_map(
        local_fn,
        mesh=grid_mesh,
        in_specs=(P(("z", "p"), None), P(("z", "p"), None), P(None, None), P(None, None), P(), P(), P(("z", "p"))),
        out_specs=(P(), P(), P(), P(None, None), P(None, None)),
        check_vma=False,
    )
```

```python
import jax
import jax.numpy as jnp
from jax import lax
from jax.experimental import pallas as pl
from jax.experimental.pallas import tpu as pltpu
from jax.sharding import Mesh, PartitionSpec as P

CONTRACT_ROWS = (((0,), (0,)), ((), ()))
LOG2E = 1.4426950408889634
LN2 = 0.6931471805599453
ROWS_TILE = 1024
COLS_TILE = 512
COLS_SUB = 256
LANES = 128


def pair_patch(sim, ids_img, ids_txt, scale2, bias2):
    sign = jnp.where(ids_img == ids_txt, -1.0, 1.0)
    return (sim * scale2 + bias2) * sign, sign


def pair_kernel(n_rows, n_steps, scal_ref, img_ref, img_t_ref, txt_ref, txt_t_ref, idi_ref, idt_ref,
                dimg_ref, dtxt_ref, sums_ref, grad_even, grad_odd):
    step = pl.program_id(0)
    prev = jnp.maximum(step - 1, 0)

    @pl.when(step == 0)
    def _():
        grad_odd[...] = jnp.zeros_like(grad_odd)
        dimg_ref[...] = jnp.zeros_like(dimg_ref)
        sums_ref[...] = jnp.zeros_like(sums_ref)

    @pl.when(lax.rem(prev, n_rows) == 0)
    def _():
        dtxt_ref[...] = jnp.zeros_like(dtxt_ref)

    row_now = pl.multiple_of(lax.rem(jnp.minimum(step, n_steps - 1), n_rows) * ROWS_TILE, ROWS_TILE)
    row_prev = pl.multiple_of(lax.rem(prev, n_rows) * ROWS_TILE, ROWS_TILE)
    scale2 = scal_ref[0]
    bias2 = scal_ref[1]
    n_sub = COLS_TILE // COLS_SUB
    per_sub = COLS_SUB // LANES

    def similarity(sub):
        return jnp.dot(img_ref[pl.ds(row_now, ROWS_TILE), :], txt_t_ref[:, sub * COLS_SUB:(sub + 1) * COLS_SUB],
                       preferred_element_type=jnp.float32)

    def again(grad_now):
        def rows_again(piece, _):
            base = pl.multiple_of(row_now + piece * 64, 64)
            rows = pl.ds(pl.multiple_of(piece * 64, 64), 64)
            for block in range(COLS_TILE // LANES):
                cols = slice(block * LANES, block * LANES + LANES)
                sim = jnp.dot(img_ref[pl.ds(base, 64), :], txt_t_ref[:, cols], preferred_element_type=jnp.float32)
                margin, sign = pair_patch(sim, idi_ref[pl.ds(base, 64), :], idt_ref[0:1, cols], scale2, bias2)
                tail = jnp.exp2(-jnp.abs(margin))
                denom = 1.0 + tail
                grad = jnp.where(margin >= 0.0, 1.0, tail) * (1.0 / denom) * sign
                loss = LN2 * jnp.maximum(margin, 0.0) + jnp.log1p(tail)
                for index, term in enumerate((loss, grad * sim, grad)):
                    sums_ref[index] += jnp.sum(term.reshape(8, 8, LANES), axis=0)
                grad_now[block, rows, :] = grad.astype(jnp.bfloat16)
            return 0

        lax.fori_loop(0, ROWS_TILE // 64, rows_again, 0)

    def tile_pair(grad_now, grad_prev):
        zero = jnp.zeros((8, LANES), jnp.float32)
        sum_log, sum_gs, sum_g, sum_top = zero, zero, zero, zero
        sim_next = similarity(0)
        for sub in range(n_sub):
            cols = slice(sub * COLS_SUB, (sub + 1) * COLS_SUB)
            sim_sub = sim_next
            old = jnp.concatenate([grad_prev[sub * per_sub + k] for k in range(per_sub)], axis=1)
            dtxt_ref[:, cols] += jnp.dot(
                img_t_ref[:, pl.ds(row_prev, ROWS_TILE)], old, preferred_element_type=jnp.float32)
            piece = ROWS_TILE // n_sub
            old = jnp.concatenate(
                [grad_prev[k, sub * piece:(sub + 1) * piece, :] for k in range(COLS_TILE // LANES)], axis=1)
            dimg_ref[pl.ds(row_prev + sub * piece, piece), :] += jnp.dot(
                old, txt_ref[...], preferred_element_type=jnp.float32)
            if sub + 1 < n_sub:
                sim_next = similarity(sub + 1)
            for row in range(0, ROWS_TILE, 16):
                for lane in range(per_sub):
                    lane0 = lane * LANES
                    idt = idt_ref[:, sub * COLS_SUB + lane0:sub * COLS_SUB + lane0 + LANES]
                    pair = []
                    for line in (row, row + 8):
                        sim = sim_sub[line:line + 8, lane0:lane0 + LANES]
                        margin, sign = pair_patch(sim, idi_ref[pl.ds(row_now + line, 8), :], idt, scale2, bias2)
                        growth = jnp.exp2(margin)
                        denom = 1.0 + growth
                        grad = growth * (1.0 / denom) * sign
                        sum_gs = sum_gs + grad * sim
                        sum_g = sum_g + grad
                        if row % 64 == 0 and line == row:
                            if lane == 0:
                                chains = [None] * per_sub
                            chains[lane] = growth
                        else:
                            chains[lane] = growth + chains[lane] * denom
                        pair.append(grad)
                    grad_now[sub * per_sub + lane, row:row + 16, :] = jnp.concatenate(pair, axis=0).astype(jnp.bfloat16)
                if row % 64 == 48:
                    for prod in chains:
                        sum_log = sum_log + jnp.log1p(prod)
                        sum_top = sum_top + prod

        live = step < n_steps
        fits = jnp.sum(sum_top) < 1e30

        @pl.when(jnp.logical_and(live, fits))
        def _():
            sums_ref[0] += sum_log
            sums_ref[1] += sum_gs
            sums_ref[2] += sum_g

        @pl.when(jnp.logical_and(live, jnp.logical_not(fits)))
        def _():
            again(grad_now)

    @pl.when(lax.rem(step, 2) == 0)
    def _():
        tile_pair(grad_even, grad_odd)

    @pl.when(lax.rem(step, 2) == 1)
    def _():
        tile_pair(grad_odd, grad_even)


def pair_call(scal, img, img_t, txt, txt_t, idi, idt):
    n_img, width = img.shape
    n_txt = txt.shape[0]
    n_rows = n_img // ROWS_TILE
    n_cols = n_txt // COLS_TILE
    n_steps = n_rows * n_cols
    once = pl.Buffered(1)

    def col_now(step):
        return jnp.minimum(step, n_steps - 1) // n_rows

    def col_prev(step):
        return jnp.maximum(step - 1, 0) // n_rows

    return pl.pallas_call(
        lambda *refs: pair_kernel(n_rows, n_steps, *refs),
        grid=(n_steps + 1,),
        in_specs=[
            pl.BlockSpec(memory_space=pltpu.SMEM),
            pl.BlockSpec((n_img, width), lambda s: (0, 0), pipeline_mode=once),
            pl.BlockSpec((width, n_img), lambda s: (0, 0), pipeline_mode=once),
            pl.BlockSpec((COLS_TILE, width), lambda s: (col_prev(s), 0)),
            pl.BlockSpec((width, COLS_TILE), lambda s: (0, col_now(s))),
            pl.BlockSpec((n_img, LANES), lambda s: (0, 0), pipeline_mode=once),
            pl.BlockSpec((8, COLS_TILE), lambda s: (0, col_now(s))),
        ],
        out_specs=[
            pl.BlockSpec((n_img, width), lambda s: (0, 0)),
            pl.BlockSpec((width, COLS_TILE), lambda s: (0, col_prev(s))),
            pl.BlockSpec((3, 8, LANES), lambda s: (0, 0, 0)),
        ],
        out_shape=[
            jax.ShapeDtypeStruct((n_img, width), jnp.float32),
            jax.ShapeDtypeStruct((width, n_txt), jnp.float32),
            jax.ShapeDtypeStruct((3, 8, LANES), jnp.float32),
        ],
        scratch_shapes=[pltpu.VMEM((COLS_TILE // LANES, ROWS_TILE, LANES), jnp.bfloat16)] * 2,
        compiler_params=pltpu.CompilerParams(
            dimension_semantics=("arbitrary",), vmem_limit_bytes=60 * 1024 * 1024),
        cost_estimate=pl.CostEstimate(
            flops=6 * n_img * n_txt * width, bytes_accessed=4 * (n_img + n_txt) * width * 2,
            transcendentals=2 * n_img * n_txt),
        name="pair_tiles",
    )(scal, img, img_t, txt, txt_t, idi, idt)


def prep_kernel(wide, n_alias, x_ref, w_ref, *refs):
    emb_ref, emb_t_ref, raw_ref, x_out = refs[n_alias:]
    x = x_ref[...]
    x_out[...] = x
    raw = jnp.dot(x, w_ref[...], preferred_element_type=jnp.float32)
    unit = raw * lax.rsqrt(jnp.sum(raw * raw, axis=1, keepdims=True))
    emb_ref[...] = unit.astype(jnp.bfloat16)
    emb_t_ref[...] = unit.T.astype(jnp.bfloat16)
    raw_ref[...] = raw.T if wide else raw


def prep_block(x, w, index, n_blocks, bufs, wide):
    n_blk, feat = x.shape[0] - ID_ROWS, x.shape[1]
    width = w.shape[1]
    tile = 256
    per = n_blk // tile
    n_all = n_blk * n_blocks
    rows = pl.BlockSpec((tile, width), lambda i: (index * per + i, 0))
    cols = pl.BlockSpec((width, tile), lambda i: (0, index * per + i))
    fixed = pl.BlockSpec(w.shape, lambda i: (0, 0))
    bufs = () if bufs is None else tuple(bufs)
    return pl.pallas_call(
        lambda *refs: prep_kernel(wide, len(bufs), *refs),
        grid=(per,),
        in_specs=[pl.BlockSpec((tile, feat), lambda i: (i, 0)), fixed]
        + [pl.BlockSpec(memory_space=pl.ANY)] * len(bufs),
        out_specs=[rows, cols, cols if wide else rows, pl.BlockSpec((tile, feat), lambda i: (index * per + i, 0))],
        out_shape=[
            jax.ShapeDtypeStruct((n_all, width), jnp.bfloat16),
            jax.ShapeDtypeStruct((width, n_all), jnp.bfloat16),
            jax.ShapeDtypeStruct((width, n_all) if wide else (n_all, width), jnp.float32),
            jax.ShapeDtypeStruct((n_all, feat), jnp.bfloat16),
        ],
        input_output_aliases={2 + k: k for k in range(len(bufs))},
        compiler_params=pltpu.CompilerParams(dimension_semantics=("arbitrary",), vmem_limit_bytes=60 * 1024 * 1024),
        cost_estimate=pl.CostEstimate(
            flops=2 * n_blk * feat * width, bytes_accessed=n_blk * (4 * feat + 8 * width), transcendentals=n_blk),
        name="prep_rows",
    )(x, w, *bufs)


def tail_kernel(wide, grad_ref, raw_ref, x_ref, out_ref, acc_ref):
    step = pl.program_id(0)
    axis = 0 if wide else 1
    raw, grad = raw_ref[...], grad_ref[...]
    inv_norm = lax.rsqrt(jnp.sum(raw * raw, axis=axis, keepdims=True))
    unit = raw * inv_norm
    raw_grad = inv_norm * (grad - unit * jnp.sum(unit * grad, axis=axis, keepdims=True))
    if not wide:
        raw_grad = raw_grad.T
    high = raw_grad.astype(jnp.bfloat16)
    low = (raw_grad - high.astype(jnp.float32)).astype(jnp.bfloat16)
    part = jnp.dot(high, x_ref[...], preferred_element_type=jnp.float32)
    part = part + jnp.dot(low, x_ref[...], preferred_element_type=jnp.float32)

    @pl.when(step == 0)
    def _():
        acc_ref[...] = part

    @pl.when(step > 0)
    def _():
        acc_ref[...] += part

    out_ref[...] = acc_ref[...]


def tail_call(grad, raw, x, wide):
    n_all, feat = x.shape
    width = grad.shape[0] if wide else grad.shape[1]
    tile = 512
    block = pl.BlockSpec((width, tile), lambda i: (0, i)) if wide else pl.BlockSpec((tile, width), lambda i: (i, 0))
    return pl.pallas_call(
        lambda *refs: tail_kernel(wide, *refs),
        grid=(n_all // tile,),
        in_specs=[block, block, pl.BlockSpec((tile, feat), lambda i: (i, 0))],
        out_specs=pl.BlockSpec((width, feat), lambda i: (0, 0)),
        out_shape=jax.ShapeDtypeStruct((width, feat), jnp.float32),
        scratch_shapes=[pltpu.VMEM((width, feat), jnp.float32)],
        compiler_params=pltpu.CompilerParams(dimension_semantics=("arbitrary",), vmem_limit_bytes=60 * 1024 * 1024),
        cost_estimate=pl.CostEstimate(
            flops=4 * n_all * feat * width, bytes_accessed=n_all * (2 * feat + 8 * width), transcendentals=n_all),
        name="tail_cols" if wide else "tail_rows",
    )(grad, raw, x)


ID_ROWS = 16
ID_BASE = 128


def pack_ids(feat, ids):
    digits = jnp.concatenate([ids // ID_BASE, lax.rem(ids, ID_BASE)]).astype(jnp.bfloat16)
    width = feat.shape[1]
    digits = jnp.pad(digits, (0, ID_ROWS * width - digits.shape[0])).reshape(ID_ROWS, width)
    return jnp.concatenate([feat, digits], axis=0)


def read_ids(block):
    rows = block.shape[0] - ID_ROWS
    digits = block[rows:].reshape(-1)[:2 * rows].astype(jnp.int32)
    return digits[:rows] * ID_BASE + digits[rows:]


def sum_over_devices(value, n_z, n_p):
    place = {"p": lax.axis_index("p"), "z": lax.axis_index("z")}
    size = {"p": n_p, "z": n_z}
    steps = [("p", 1), ("p", 2), ("p", 4), ("z", 1), ("z", 2)]

    def swap(part, axis, mask):
        return lax.ppermute(part, axis, [(src, src ^ mask) for src in range(size[axis])])

    for axis, mask in steps:
        half = value.shape[0] // 2
        upper = jnp.bitwise_and(place[axis], mask) // mask
        keep = lax.dynamic_slice_in_dim(value, upper * half, half)
        send = lax.dynamic_slice_in_dim(value, (1 - upper) * half, half)
        value = keep + swap(send, axis, mask)
    for axis, mask in reversed(steps):
        upper = jnp.bitwise_and(place[axis], mask) > 0
        other = swap(value, axis, mask)
        value = jnp.where(upper, jnp.concatenate([other, value]), jnp.concatenate([value, other]))
    return value


def solution(mesh):
    n_dev = mesh.shape["data"]
    n_z = 4
    n_p = n_dev // n_z
    grid_mesh = Mesh(mesh.devices.reshape(n_z, n_p), ("z", "p"))

    def rotate(value, hop):
        return lax.ppermute(value, "z", [(src, (src + hop) % n_z) for src in range(n_z)])

    def swap(value, mask):
        return lax.ppermute(value, "p", [(src, src ^ mask) for src in range(n_p)])

    def local_fn(feat_img, feat_txt, w_img, w_txt, log_temp, logit_bias, pair_ids):
        total_rows = feat_img.shape[0] * n_dev
        temp_scale = jnp.exp(log_temp)
        own_txt, own_img = pack_ids(feat_txt, pair_ids), pack_ids(feat_img, pair_ids)
        txt_blocks = [own_txt] + [rotate(own_txt, hop) for hop in (1, 3, 2)]
        img_blocks = []
        for mask in range(0, n_p, 2):
            same_core = own_img if mask == 0 else swap(own_img, mask)
            img_blocks += [same_core, swap(same_core, 1)]
        ids_txt = jnp.concatenate([read_ids(block) for block in txt_blocks])
        ids_img = jnp.concatenate([read_ids(block) for block in img_blocks])
        id_rows = jnp.broadcast_to(ids_txt[:, None], (ids_txt.shape[0], LANES))
        id_cols = jnp.broadcast_to(ids_img[None, :], (8, ids_img.shape[0]))

        txt_all = None
        for index, block in enumerate(txt_blocks):
            txt_all = prep_block(block, w_txt, index, n_z, txt_all, False)
        img_all = None
        for index, block in enumerate(img_blocks):
            img_all = prep_block(block, w_img, index, n_p, img_all, True)
        emb_txt, emb_txt_t, raw_txt, x_txt = txt_all
        emb_img, emb_img_t, raw_img_t, x_img = img_all
        scal = jnp.stack([temp_scale * LOG2E, logit_bias * LOG2E])
        part_txt, part_img_t, sums = pair_call(scal, emb_txt, emb_txt_t, emb_img, emb_img_t, id_rows, id_cols)
        dw_txt_t = tail_call(part_txt, raw_txt, x_txt, False)
        dw_img_t = tail_call(part_img_t, raw_img_t, x_img, True)
        sums = jnp.sum(sums, axis=(1, 2)) / total_rows
        sums = jnp.broadcast_to(jnp.pad(sums, (0, dw_txt_t.shape[0] - 3))[:, None], (dw_txt_t.shape[0], LANES))
        total = sum_over_devices(jnp.concatenate([dw_img_t, dw_txt_t, sums], axis=1), n_z, n_p)
        scale = temp_scale / total_rows
        n_img = dw_img_t.shape[1]
        n_both = n_img + dw_txt_t.shape[1]
        sums = total[:3, n_both]
        return (sums[0], temp_scale * sums[1], sums[2],
                scale * total[:, :n_img].T, scale * total[:, n_img:n_both].T)

    return jax.shard_map(
        local_fn,
        mesh=grid_mesh,
        in_specs=(P(("z", "p"), None), P(("z", "p"), None), P(None, None), P(None, None), P(), P(), P(("z", "p"))),
        out_specs=(P(), P(), P(), P(None, None), P(None, None)),
        check_vma=False,
    )
```

```python
import jax
import jax.numpy as jnp
from jax import lax
from jax.experimental import pallas as pl
from jax.experimental.pallas import tpu as pltpu
from jax.sharding import Mesh, PartitionSpec as P

CONTRACT_ROWS = (((0,), (0,)), ((), ()))
LOG2E = 1.4426950408889634
LN2 = 0.6931471805599453
ROWS_TILE = 1024
COLS_TILE = 512
COLS_SUB = 256
LANES = 128


def pair_patch(sim, ids_img, ids_txt, scale2, bias2):
    sign = jnp.where(ids_img == ids_txt, -1.0, 1.0)
    return (sim * scale2 + bias2) * sign, sign


def pair_kernel(n_rows, n_steps, scal_ref, img_ref, img_t_ref, txt_ref, txt_t_ref, idi_ref, idt_ref,
                dimg_ref, dtxt_ref, sums_ref, grad_even, grad_odd):
    step = pl.program_id(0)
    prev = jnp.maximum(step - 1, 0)

    @pl.when(step == 0)
    def _():
        grad_odd[...] = jnp.zeros_like(grad_odd)
        dimg_ref[...] = jnp.zeros_like(dimg_ref)
        sums_ref[...] = jnp.zeros_like(sums_ref)

    @pl.when(lax.rem(prev, n_rows) == 0)
    def _():
        dtxt_ref[...] = jnp.zeros_like(dtxt_ref)

    row_now = pl.multiple_of(lax.rem(jnp.minimum(step, n_steps - 1), n_rows) * ROWS_TILE, ROWS_TILE)
    row_prev = pl.multiple_of(lax.rem(prev, n_rows) * ROWS_TILE, ROWS_TILE)
    scale2 = scal_ref[0]
    bias2 = scal_ref[1]
    n_sub = COLS_TILE // COLS_SUB
    per_sub = COLS_SUB // LANES

    def similarity(sub):
        return jnp.dot(img_ref[pl.ds(row_now, ROWS_TILE), :], txt_t_ref[:, sub * COLS_SUB:(sub + 1) * COLS_SUB],
                       preferred_element_type=jnp.float32)

    def again(grad_now):
        def rows_again(piece, _):
            base = pl.multiple_of(row_now + piece * 64, 64)
            rows = pl.ds(pl.multiple_of(piece * 64, 64), 64)
            for block in range(COLS_TILE // LANES):
                cols = slice(block * LANES, block * LANES + LANES)
                sim = jnp.dot(img_ref[pl.ds(base, 64), :], txt_t_ref[:, cols], preferred_element_type=jnp.float32)
                margin, sign = pair_patch(sim, idi_ref[pl.ds(base, 64), :], idt_ref[0:1, cols], scale2, bias2)
                tail = jnp.exp2(-jnp.abs(margin))
                denom = 1.0 + tail
                grad = jnp.where(margin >= 0.0, 1.0, tail) * (1.0 / denom) * sign
                loss = LN2 * jnp.maximum(margin, 0.0) + jnp.log1p(tail)
                for index, term in enumerate((loss, grad * sim, grad)):
                    sums_ref[index] += jnp.sum(term.reshape(8, 8, LANES), axis=0)
                grad_now[block, rows, :] = grad.astype(jnp.bfloat16)
            return 0

        lax.fori_loop(0, ROWS_TILE // 64, rows_again, 0)

    def tile_pair(grad_now, grad_prev):
        zero = jnp.zeros((8, LANES), jnp.float32)
        sum_log, sum_gs, sum_g, sum_top = zero, zero, zero, zero
        sim_next = similarity(0)
        for sub in range(n_sub):
            cols = slice(sub * COLS_SUB, (sub + 1) * COLS_SUB)
            sim_sub = sim_next
            old = jnp.concatenate([grad_prev[sub * per_sub + k] for k in range(per_sub)], axis=1)
            dtxt_ref[:, cols] += jnp.dot(
                img_t_ref[:, pl.ds(row_prev, ROWS_TILE)], old, preferred_element_type=jnp.float32)
            piece = ROWS_TILE // n_sub
            old = jnp.concatenate(
                [grad_prev[k, sub * piece:(sub + 1) * piece, :] for k in range(COLS_TILE // LANES)], axis=1)
            dimg_ref[pl.ds(row_prev + sub * piece, piece), :] += jnp.dot(
                old, txt_ref[...], preferred_element_type=jnp.float32)
            if sub + 1 < n_sub:
                sim_next = similarity(sub + 1)
            for row in range(0, ROWS_TILE, 16):
                for lane in range(per_sub):
                    lane0 = lane * LANES
                    idt = idt_ref[:, sub * COLS_SUB + lane0:sub * COLS_SUB + lane0 + LANES]
                    pair = []
                    for line in (row, row + 8):
                        sim = sim_sub[line:line + 8, lane0:lane0 + LANES]
                        margin, sign = pair_patch(sim, idi_ref[pl.ds(row_now + line, 8), :], idt, scale2, bias2)
                        growth = jnp.exp2(margin)
                        denom = 1.0 + growth
                        grad = growth * (1.0 / denom) * sign
                        sum_gs = sum_gs + grad * sim
                        sum_g = sum_g + grad
                        if row % 128 == 0 and line == row:
                            if lane == 0:
                                chains = [None] * per_sub
                            chains[lane] = growth
                        else:
                            chains[lane] = growth + chains[lane] * denom
                        pair.append(grad)
                    grad_now[sub * per_sub + lane, row:row + 16, :] = jnp.concatenate(pair, axis=0).astype(jnp.bfloat16)
                if row % 128 == 112:
                    for prod in chains:
                        sum_log = sum_log + jnp.log1p(prod)
                        sum_top = sum_top + prod

        live = step < n_steps
        fits = jnp.sum(sum_top) < 1e30

        @pl.when(jnp.logical_and(live, fits))
        def _():
            sums_ref[0] += sum_log
            sums_ref[1] += sum_gs
            sums_ref[2] += sum_g

        @pl.when(jnp.logical_and(live, jnp.logical_not(fits)))
        def _():
            again(grad_now)

    @pl.when(lax.rem(step, 2) == 0)
    def _():
        tile_pair(grad_even, grad_odd)

    @pl.when(lax.rem(step, 2) == 1)
    def _():
        tile_pair(grad_odd, grad_even)


def pair_call(scal, img, img_t, txt, txt_t, idi, idt):
    n_img, width = img.shape
    n_txt = txt.shape[0]
    n_rows = n_img // ROWS_TILE
    n_cols = n_txt // COLS_TILE
    n_steps = n_rows * n_cols
    once = pl.Buffered(1)

    def col_now(step):
        return jnp.minimum(step, n_steps - 1) // n_rows

    def col_prev(step):
        return jnp.maximum(step - 1, 0) // n_rows

    return pl.pallas_call(
        lambda *refs: pair_kernel(n_rows, n_steps, *refs),
        grid=(n_steps + 1,),
        in_specs=[
            pl.BlockSpec(memory_space=pltpu.SMEM),
            pl.BlockSpec((n_img, width), lambda s: (0, 0), pipeline_mode=once),
            pl.BlockSpec((width, n_img), lambda s: (0, 0), pipeline_mode=once),
            pl.BlockSpec((COLS_TILE, width), lambda s: (col_prev(s), 0)),
            pl.BlockSpec((width, COLS_TILE), lambda s: (0, col_now(s))),
            pl.BlockSpec((n_img, LANES), lambda s: (0, 0), pipeline_mode=once),
            pl.BlockSpec((8, COLS_TILE), lambda s: (0, col_now(s))),
        ],
        out_specs=[
            pl.BlockSpec((n_img, width), lambda s: (0, 0)),
            pl.BlockSpec((width, COLS_TILE), lambda s: (0, col_prev(s))),
            pl.BlockSpec((3, 8, LANES), lambda s: (0, 0, 0)),
        ],
        out_shape=[
            jax.ShapeDtypeStruct((n_img, width), jnp.float32),
            jax.ShapeDtypeStruct((width, n_txt), jnp.float32),
            jax.ShapeDtypeStruct((3, 8, LANES), jnp.float32),
        ],
        scratch_shapes=[pltpu.VMEM((COLS_TILE // LANES, ROWS_TILE, LANES), jnp.bfloat16)] * 2,
        compiler_params=pltpu.CompilerParams(
            dimension_semantics=("arbitrary",), vmem_limit_bytes=60 * 1024 * 1024),
        cost_estimate=pl.CostEstimate(
            flops=6 * n_img * n_txt * width, bytes_accessed=4 * (n_img + n_txt) * width * 2,
            transcendentals=2 * n_img * n_txt),
        name="pair_tiles",
    )(scal, img, img_t, txt, txt_t, idi, idt)


def prep_kernel(wide, n_alias, x_ref, w_ref, *refs):
    emb_ref, emb_t_ref, raw_ref, x_out = refs[n_alias:]
    x = x_ref[...]
    x_out[...] = x
    raw = jnp.dot(x, w_ref[...], preferred_element_type=jnp.float32)
    unit = raw * lax.rsqrt(jnp.sum(raw * raw, axis=1, keepdims=True))
    emb_ref[...] = unit.astype(jnp.bfloat16)
    emb_t_ref[...] = unit.T.astype(jnp.bfloat16)
    raw_ref[...] = raw.T if wide else raw


def prep_block(x, w, index, n_blocks, bufs, wide):
    n_blk, feat = x.shape[0] - ID_ROWS, x.shape[1]
    width = w.shape[1]
    tile = 256
    per = n_blk // tile
    n_all = n_blk * n_blocks
    rows = pl.BlockSpec((tile, width), lambda i: (index * per + i, 0))
    cols = pl.BlockSpec((width, tile), lambda i: (0, index * per + i))
    fixed = pl.BlockSpec(w.shape, lambda i: (0, 0))
    bufs = () if bufs is None else tuple(bufs)
    return pl.pallas_call(
        lambda *refs: prep_kernel(wide, len(bufs), *refs),
        grid=(per,),
        in_specs=[pl.BlockSpec((tile, feat), lambda i: (i, 0)), fixed]
        + [pl.BlockSpec(memory_space=pl.ANY)] * len(bufs),
        out_specs=[rows, cols, cols if wide else rows, pl.BlockSpec((tile, feat), lambda i: (index * per + i, 0))],
        out_shape=[
            jax.ShapeDtypeStruct((n_all, width), jnp.bfloat16),
            jax.ShapeDtypeStruct((width, n_all), jnp.bfloat16),
            jax.ShapeDtypeStruct((width, n_all) if wide else (n_all, width), jnp.float32),
            jax.ShapeDtypeStruct((n_all, feat), jnp.bfloat16),
        ],
        input_output_aliases={2 + k: k for k in range(len(bufs))},
        compiler_params=pltpu.CompilerParams(dimension_semantics=("arbitrary",), vmem_limit_bytes=60 * 1024 * 1024),
        cost_estimate=pl.CostEstimate(
            flops=2 * n_blk * feat * width, bytes_accessed=n_blk * (4 * feat + 8 * width), transcendentals=n_blk),
        name="prep_rows",
    )(x, w, *bufs)


def tail_kernel(wide, grad_ref, raw_ref, x_ref, out_ref, acc_ref):
    step = pl.program_id(0)
    axis = 0 if wide else 1
    raw, grad = raw_ref[...], grad_ref[...]
    inv_norm = lax.rsqrt(jnp.sum(raw * raw, axis=axis, keepdims=True))
    unit = raw * inv_norm
    raw_grad = inv_norm * (grad - unit * jnp.sum(unit * grad, axis=axis, keepdims=True))
    if not wide:
        raw_grad = raw_grad.T
    high = raw_grad.astype(jnp.bfloat16)
    low = (raw_grad - high.astype(jnp.float32)).astype(jnp.bfloat16)
    part = jnp.dot(high, x_ref[...], preferred_element_type=jnp.float32)
    part = part + jnp.dot(low, x_ref[...], preferred_element_type=jnp.float32)

    @pl.when(step == 0)
    def _():
        acc_ref[...] = part

    @pl.when(step > 0)
    def _():
        acc_ref[...] += part

    out_ref[...] = acc_ref[...]


def tail_call(grad, raw, x, wide):
    n_all, feat = x.shape
    width = grad.shape[0] if wide else grad.shape[1]
    tile = 512
    block = pl.BlockSpec((width, tile), lambda i: (0, i)) if wide else pl.BlockSpec((tile, width), lambda i: (i, 0))
    return pl.pallas_call(
        lambda *refs: tail_kernel(wide, *refs),
        grid=(n_all // tile,),
        in_specs=[block, block, pl.BlockSpec((tile, feat), lambda i: (i, 0))],
        out_specs=pl.BlockSpec((width, feat), lambda i: (0, 0)),
        out_shape=jax.ShapeDtypeStruct((width, feat), jnp.float32),
        scratch_shapes=[pltpu.VMEM((width, feat), jnp.float32)],
        compiler_params=pltpu.CompilerParams(dimension_semantics=("arbitrary",), vmem_limit_bytes=60 * 1024 * 1024),
        cost_estimate=pl.CostEstimate(
            flops=4 * n_all * feat * width, bytes_accessed=n_all * (2 * feat + 8 * width), transcendentals=n_all),
        name="tail_cols" if wide else "tail_rows",
    )(grad, raw, x)


ID_ROWS = 16
ID_BASE = 128


def pack_ids(feat, ids):
    digits = jnp.concatenate([ids // ID_BASE, lax.rem(ids, ID_BASE)]).astype(jnp.bfloat16)
    width = feat.shape[1]
    digits = jnp.pad(digits, (0, ID_ROWS * width - digits.shape[0])).reshape(ID_ROWS, width)
    return jnp.concatenate([feat, digits], axis=0)


def read_ids(block):
    rows = block.shape[0] - ID_ROWS
    digits = block[rows:].reshape(-1)[:2 * rows].astype(jnp.int32)
    return digits[:rows] * ID_BASE + digits[rows:]


def sum_over_devices(value, n_z, n_p):
    place = {"p": lax.axis_index("p"), "z": lax.axis_index("z")}
    size = {"p": n_p, "z": n_z}
    steps = [("p", 1), ("p", 2), ("p", 4), ("z", 1), ("z", 2)]

    def swap(part, axis, mask):
        return lax.ppermute(part, axis, [(src, src ^ mask) for src in range(size[axis])])

    for axis, mask in steps:
        half = value.shape[0] // 2
        upper = jnp.bitwise_and(place[axis], mask) // mask
        keep = lax.dynamic_slice_in_dim(value, upper * half, half)
        send = lax.dynamic_slice_in_dim(value, (1 - upper) * half, half)
        value = keep + swap(send, axis, mask)
    for axis, mask in reversed(steps):
        upper = jnp.bitwise_and(place[axis], mask) > 0
        other = swap(value, axis, mask)
        value = jnp.where(upper, jnp.concatenate([other, value]), jnp.concatenate([value, other]))
    return value


def solution(mesh):
    n_dev = mesh.shape["data"]
    n_z = 4
    n_p = n_dev // n_z
    grid_mesh = Mesh(mesh.devices.reshape(n_z, n_p), ("z", "p"))

    def rotate(value, hop):
        return lax.ppermute(value, "z", [(src, (src + hop) % n_z) for src in range(n_z)])

    def swap(value, mask):
        return lax.ppermute(value, "p", [(src, src ^ mask) for src in range(n_p)])

    def local_fn(feat_img, feat_txt, w_img, w_txt, log_temp, logit_bias, pair_ids):
        total_rows = feat_img.shape[0] * n_dev
        temp_scale = jnp.exp(log_temp)
        own_txt, own_img = pack_ids(feat_txt, pair_ids), pack_ids(feat_img, pair_ids)
        txt_blocks = [own_txt] + [rotate(own_txt, hop) for hop in (1, 3, 2)]
        same_core = [own_img] + [swap(own_img, mask) for mask in range(2, n_p, 2)]
        other_core = [swap(block, 1) for block in same_core]
        img_blocks = [own_img, other_core[0]] + same_core[1:] + other_core[1:]
        img_all = None
        for index, block in enumerate(img_blocks):
            img_all = prep_block(block, w_img, index, n_p, img_all, True)
        held = lax.optimization_barrier((*txt_blocks[1:], img_all[1]))
        txt_blocks = [own_txt, *held[:-1]]
        img_all = (img_all[0], held[-1], *img_all[2:])
        ids_txt = jnp.concatenate([read_ids(block) for block in txt_blocks])
        ids_img = jnp.concatenate([read_ids(block) for block in img_blocks])
        id_rows = jnp.broadcast_to(ids_txt[:, None], (ids_txt.shape[0], LANES))
        id_cols = jnp.broadcast_to(ids_img[None, :], (8, ids_img.shape[0]))

        txt_all = None
        for index, block in enumerate(txt_blocks):
            txt_all = prep_block(block, w_txt, index, n_z, txt_all, False)
        emb_txt, emb_txt_t, raw_txt, x_txt = txt_all
        emb_img, emb_img_t, raw_img_t, x_img = img_all
        scal = jnp.stack([temp_scale * LOG2E, logit_bias * LOG2E])
        part_txt, part_img_t, sums = pair_call(scal, emb_txt, emb_txt_t, emb_img, emb_img_t, id_rows, id_cols)
        dw_txt_t = tail_call(part_txt, raw_txt, x_txt, False)
        dw_img_t = tail_call(part_img_t, raw_img_t, x_img, True)
        sums = jnp.sum(sums, axis=(1, 2)) / total_rows
        sums = jnp.broadcast_to(jnp.pad(sums, (0, dw_txt_t.shape[0] - 3))[:, None], (dw_txt_t.shape[0], LANES))
        total = sum_over_devices(jnp.concatenate([dw_img_t, dw_txt_t, sums], axis=1), n_z, n_p)
        scale = temp_scale / total_rows
        n_img = dw_img_t.shape[1]
        n_both = n_img + dw_txt_t.shape[1]
        sums = total[:3, n_both]
        return (sums[0], temp_scale * sums[1], sums[2],
                scale * total[:, :n_img].T, scale * total[:, n_img:n_both].T)

    return jax.shard_map(
        local_fn,
        mesh=grid_mesh,
        in_specs=(P(("z", "p"), None), P(("z", "p"), None), P(None, None), P(None, None), P(), P(), P(("z", "p"))),
        out_specs=(P(), P(), P(), P(None, None), P(None, None)),
        check_vma=False,
    )
```

```python
import jax
import jax.numpy as jnp
from jax import lax
from jax.experimental import pallas as pl
from jax.experimental.pallas import tpu as pltpu
from jax.sharding import Mesh, PartitionSpec as P

CONTRACT_ROWS = (((0,), (0,)), ((), ()))
LOG2E = 1.4426950408889634
LN2 = 0.6931471805599453
ROWS_TILE = 1024
COLS_TILE = 512
COLS_SUB = 256
LANES = 128


def pair_patch(sim, ids_img, ids_txt, scale2, bias2):
    sign = jnp.where(ids_img == ids_txt, -1.0, 1.0)
    return (sim * scale2 + bias2) * sign, sign


def pair_kernel(n_rows, n_steps, scal_ref, img_ref, img_t_ref, txt_ref, txt_t_ref, idi_ref, idt_ref,
                dimg_ref, dtxt_ref, sums_ref, grad_even, grad_odd):
    step = pl.program_id(0)
    prev = jnp.maximum(step - 1, 0)

    @pl.when(step == 0)
    def _():
        grad_odd[...] = jnp.zeros_like(grad_odd)
        dimg_ref[...] = jnp.zeros_like(dimg_ref)
        sums_ref[...] = jnp.zeros_like(sums_ref)

    @pl.when(lax.rem(prev, n_rows) == 0)
    def _():
        dtxt_ref[...] = jnp.zeros_like(dtxt_ref)

    row_now = pl.multiple_of(lax.rem(jnp.minimum(step, n_steps - 1), n_rows) * ROWS_TILE, ROWS_TILE)
    row_prev = pl.multiple_of(lax.rem(prev, n_rows) * ROWS_TILE, ROWS_TILE)
    scale2 = scal_ref[0]
    bias2 = scal_ref[1]
    n_sub = COLS_TILE // COLS_SUB
    per_sub = COLS_SUB // LANES

    def similarity(sub):
        return jnp.dot(img_ref[pl.ds(row_now, ROWS_TILE), :], txt_t_ref[:, sub * COLS_SUB:(sub + 1) * COLS_SUB],
                       preferred_element_type=jnp.float32)

    def again(grad_now):
        def rows_again(piece, _):
            base = pl.multiple_of(row_now + piece * 64, 64)
            rows = pl.ds(pl.multiple_of(piece * 64, 64), 64)
            for block in range(COLS_TILE // LANES):
                cols = slice(block * LANES, block * LANES + LANES)
                sim = jnp.dot(img_ref[pl.ds(base, 64), :], txt_t_ref[:, cols], preferred_element_type=jnp.float32)
                margin, sign = pair_patch(sim, idi_ref[pl.ds(base, 64), :], idt_ref[0:1, cols], scale2, bias2)
                tail = jnp.exp2(-jnp.abs(margin))
                denom = 1.0 + tail
                grad = jnp.where(margin >= 0.0, 1.0, tail) * (1.0 / denom) * sign
                loss = LN2 * jnp.maximum(margin, 0.0) + jnp.log1p(tail)
                for index, term in enumerate((loss, grad * sim, grad)):
                    sums_ref[index] += jnp.sum(term.reshape(8, 8, LANES), axis=0)
                grad_now[block, rows, :] = grad.astype(jnp.bfloat16)
            return 0

        lax.fori_loop(0, ROWS_TILE // 64, rows_again, 0)

    def tile_pair(grad_now, grad_prev):
        zero = jnp.zeros((8, LANES), jnp.float32)
        sum_log, sum_gs, sum_g, sum_top = zero, zero, zero, zero
        sim_next = similarity(0)
        for sub in range(n_sub):
            cols = slice(sub * COLS_SUB, (sub + 1) * COLS_SUB)
            sim_sub = sim_next
            old = jnp.concatenate([grad_prev[sub * per_sub + k] for k in range(per_sub)], axis=1)
            dtxt_ref[:, cols] += jnp.dot(
                img_t_ref[:, pl.ds(row_prev, ROWS_TILE)], old, preferred_element_type=jnp.float32)
            piece = ROWS_TILE // n_sub
            old = jnp.concatenate(
                [grad_prev[k, sub * piece:(sub + 1) * piece, :] for k in range(COLS_TILE // LANES)], axis=1)
            dimg_ref[pl.ds(row_prev + sub * piece, piece), :] += jnp.dot(
                old, txt_ref[...], preferred_element_type=jnp.float32)
            if sub + 1 < n_sub:
                sim_next = similarity(sub + 1)
            for row in range(0, ROWS_TILE, 16):
                for lane in range(per_sub):
                    lane0 = lane * LANES
                    idt = idt_ref[:, sub * COLS_SUB + lane0:sub * COLS_SUB + lane0 + LANES]
                    pair = []
                    for line in (row, row + 8):
                        sim = sim_sub[line:line + 8, lane0:lane0 + LANES]
                        margin, sign = pair_patch(sim, idi_ref[pl.ds(row_now + line, 8), :], idt, scale2, bias2)
                        growth = jnp.exp2(margin)
                        denom = 1.0 + growth
                        grad = growth * (1.0 / denom) * sign
                        sum_gs = sum_gs + grad * sim
                        sum_g = sum_g + grad
                        if row % 128 == 0 and line == row:
                            if lane == 0:
                                chains = [None] * per_sub
                            chains[lane] = growth
                        else:
                            chains[lane] = growth + chains[lane] * denom
                        pair.append(grad)
                    grad_now[sub * per_sub + lane, row:row + 16, :] = jnp.concatenate(pair, axis=0).astype(jnp.bfloat16)
                if row % 128 == 112:
                    for prod in chains:
                        sum_log = sum_log + jnp.log1p(prod)
                        sum_top = sum_top + prod

        live = step < n_steps
        fits = jnp.sum(sum_top) < 1e30

        @pl.when(jnp.logical_and(live, fits))
        def _():
            sums_ref[0] += sum_log
            sums_ref[1] += sum_gs
            sums_ref[2] += sum_g

        @pl.when(jnp.logical_and(live, jnp.logical_not(fits)))
        def _():
            again(grad_now)

    @pl.when(lax.rem(step, 2) == 0)
    def _():
        tile_pair(grad_even, grad_odd)

    @pl.when(lax.rem(step, 2) == 1)
    def _():
        tile_pair(grad_odd, grad_even)


def pair_call(scal, img, img_t, txt, txt_t, idi, idt):
    n_img, width = img.shape
    n_txt = txt.shape[0]
    n_rows = n_img // ROWS_TILE
    n_cols = n_txt // COLS_TILE
    n_steps = n_rows * n_cols
    once = pl.Buffered(1)

    def col_now(step):
        return jnp.minimum(step, n_steps - 1) // n_rows

    def col_prev(step):
        return jnp.maximum(step - 1, 0) // n_rows

    return pl.pallas_call(
        lambda *refs: pair_kernel(n_rows, n_steps, *refs),
        grid=(n_steps + 1,),
        in_specs=[
            pl.BlockSpec(memory_space=pltpu.SMEM),
            pl.BlockSpec((n_img, width), lambda s: (0, 0), pipeline_mode=once),
            pl.BlockSpec((width, n_img), lambda s: (0, 0), pipeline_mode=once),
            pl.BlockSpec((COLS_TILE, width), lambda s: (col_prev(s), 0)),
            pl.BlockSpec((width, COLS_TILE), lambda s: (0, col_now(s))),
            pl.BlockSpec((n_img, LANES), lambda s: (0, 0), pipeline_mode=once),
            pl.BlockSpec((8, COLS_TILE), lambda s: (0, col_now(s))),
        ],
        out_specs=[
            pl.BlockSpec((n_img, width), lambda s: (0, 0)),
            pl.BlockSpec((width, COLS_TILE), lambda s: (0, col_prev(s))),
            pl.BlockSpec((3, 8, LANES), lambda s: (0, 0, 0)),
        ],
        out_shape=[
            jax.ShapeDtypeStruct((n_img, width), jnp.float32),
            jax.ShapeDtypeStruct((width, n_txt), jnp.float32),
            jax.ShapeDtypeStruct((3, 8, LANES), jnp.float32),
        ],
        scratch_shapes=[pltpu.VMEM((COLS_TILE // LANES, ROWS_TILE, LANES), jnp.bfloat16)] * 2,
        compiler_params=pltpu.CompilerParams(
            dimension_semantics=("arbitrary",), vmem_limit_bytes=60 * 1024 * 1024),
        cost_estimate=pl.CostEstimate(
            flops=6 * n_img * n_txt * width, bytes_accessed=4 * (n_img + n_txt) * width * 2,
            transcendentals=2 * n_img * n_txt),
        name="pair_tiles",
    )(scal, img, img_t, txt, txt_t, idi, idt)


def prep_kernel(wide, n_alias, x_ref, w_ref, *refs):
    emb_ref, emb_t_ref, raw_ref, x_out = refs[n_alias:]
    x = x_ref[...]
    x_out[...] = x
    raw = jnp.dot(x, w_ref[...], preferred_element_type=jnp.float32)
    unit = raw * lax.rsqrt(jnp.sum(raw * raw, axis=1, keepdims=True))
    emb_ref[...] = unit.astype(jnp.bfloat16)
    emb_t_ref[...] = unit.T.astype(jnp.bfloat16)
    raw_ref[...] = raw.T if wide else raw


def prep_block(x, w, index, n_blocks, bufs, wide):
    n_blk, feat = x.shape[0] - ID_ROWS, x.shape[1]
    width = w.shape[1]
    tile = 256
    per = n_blk // tile
    n_all = n_blk * n_blocks
    rows = pl.BlockSpec((tile, width), lambda i: (index * per + i, 0))
    cols = pl.BlockSpec((width, tile), lambda i: (0, index * per + i))
    fixed = pl.BlockSpec(w.shape, lambda i: (0, 0))
    bufs = () if bufs is None else tuple(bufs)
    return pl.pallas_call(
        lambda *refs: prep_kernel(wide, len(bufs), *refs),
        grid=(per,),
        in_specs=[pl.BlockSpec((tile, feat), lambda i: (i, 0)), fixed]
        + [pl.BlockSpec(memory_space=pl.ANY)] * len(bufs),
        out_specs=[rows, cols, cols if wide else rows, pl.BlockSpec((tile, feat), lambda i: (index * per + i, 0))],
        out_shape=[
            jax.ShapeDtypeStruct((n_all, width), jnp.bfloat16),
            jax.ShapeDtypeStruct((width, n_all), jnp.bfloat16),
            jax.ShapeDtypeStruct((width, n_all) if wide else (n_all, width), jnp.float32),
            jax.ShapeDtypeStruct((n_all, feat), jnp.bfloat16),
        ],
        input_output_aliases={2 + k: k for k in range(len(bufs))},
        compiler_params=pltpu.CompilerParams(dimension_semantics=("arbitrary",), vmem_limit_bytes=60 * 1024 * 1024),
        cost_estimate=pl.CostEstimate(
            flops=2 * n_blk * feat * width, bytes_accessed=n_blk * (4 * feat + 8 * width), transcendentals=n_blk),
        name="prep_rows",
    )(x, w, *bufs)


def tail_kernel(wide, grad_ref, raw_ref, x_ref, out_ref, acc_ref):
    step = pl.program_id(0)
    axis = 0 if wide else 1
    raw, grad = raw_ref[...], grad_ref[...]
    inv_norm = lax.rsqrt(jnp.sum(raw * raw, axis=axis, keepdims=True))
    unit = raw * inv_norm
    raw_grad = inv_norm * (grad - unit * jnp.sum(unit * grad, axis=axis, keepdims=True))
    if not wide:
        raw_grad = raw_grad.T
    high = raw_grad.astype(jnp.bfloat16)
    low = (raw_grad - high.astype(jnp.float32)).astype(jnp.bfloat16)
    part = jnp.dot(high, x_ref[...], preferred_element_type=jnp.float32)
    part = part + jnp.dot(low, x_ref[...], preferred_element_type=jnp.float32)

    @pl.when(step == 0)
    def _():
        acc_ref[...] = part

    @pl.when(step > 0)
    def _():
        acc_ref[...] += part

    out_ref[...] = acc_ref[...]


def tail_call(grad, raw, x, wide):
    n_all, feat = x.shape
    width = grad.shape[0] if wide else grad.shape[1]
    tile = 1024
    block = pl.BlockSpec((width, tile), lambda i: (0, i)) if wide else pl.BlockSpec((tile, width), lambda i: (i, 0))
    return pl.pallas_call(
        lambda *refs: tail_kernel(wide, *refs),
        grid=(n_all // tile,),
        in_specs=[block, block, pl.BlockSpec((tile, feat), lambda i: (i, 0))],
        out_specs=pl.BlockSpec((width, feat), lambda i: (0, 0)),
        out_shape=jax.ShapeDtypeStruct((width, feat), jnp.float32),
        scratch_shapes=[pltpu.VMEM((width, feat), jnp.float32)],
        compiler_params=pltpu.CompilerParams(dimension_semantics=("arbitrary",), vmem_limit_bytes=60 * 1024 * 1024),
        cost_estimate=pl.CostEstimate(
            flops=4 * n_all * feat * width, bytes_accessed=n_all * (2 * feat + 8 * width), transcendentals=n_all),
        name="tail_cols" if wide else "tail_rows",
    )(grad, raw, x)


ID_ROWS = 16
ID_BASE = 128


def pack_ids(feat, ids):
    digits = jnp.concatenate([ids // ID_BASE, lax.rem(ids, ID_BASE)]).astype(jnp.bfloat16)
    width = feat.shape[1]
    digits = jnp.pad(digits, (0, ID_ROWS * width - digits.shape[0])).reshape(ID_ROWS, width)
    return jnp.concatenate([feat, digits], axis=0)


def read_ids(block):
    rows = block.shape[0] - ID_ROWS
    digits = block[rows:].reshape(-1)[:2 * rows].astype(jnp.int32)
    return digits[:rows] * ID_BASE + digits[rows:]


def sum_over_devices(value, n_z, n_p):
    place = {"p": lax.axis_index("p"), "z": lax.axis_index("z")}
    size = {"p": n_p, "z": n_z}
    steps = [("p", 1), ("p", 2), ("p", 4), ("z", 1), ("z", 2)]

    def swap(part, axis, mask):
        return lax.ppermute(part, axis, [(src, src ^ mask) for src in range(size[axis])])

    for axis, mask in steps:
        half = value.shape[0] // 2
        upper = jnp.bitwise_and(place[axis], mask) // mask
        keep = lax.dynamic_slice_in_dim(value, upper * half, half)
        send = lax.dynamic_slice_in_dim(value, (1 - upper) * half, half)
        value = keep + swap(send, axis, mask)
    for axis, mask in reversed(steps):
        upper = jnp.bitwise_and(place[axis], mask) > 0
        other = swap(value, axis, mask)
        value = jnp.where(upper, jnp.concatenate([other, value]), jnp.concatenate([value, other]))
    return value


def solution(mesh):
    n_dev = mesh.shape["data"]
    n_z = 4
    n_p = n_dev // n_z
    grid_mesh = Mesh(mesh.devices.reshape(n_z, n_p), ("z", "p"))

    def rotate(value, hop):
        return lax.ppermute(value, "z", [(src, (src + hop) % n_z) for src in range(n_z)])

    def swap(value, mask):
        return lax.ppermute(value, "p", [(src, src ^ mask) for src in range(n_p)])

    def local_fn(feat_img, feat_txt, w_img, w_txt, log_temp, logit_bias, pair_ids):
        total_rows = feat_img.shape[0] * n_dev
        temp_scale = jnp.exp(log_temp)
        own_txt, own_img = pack_ids(feat_txt, pair_ids), pack_ids(feat_img, pair_ids)
        txt_blocks = [own_txt] + [rotate(own_txt, hop) for hop in (1, 3, 2)]
        same_core = [own_img] + [swap(own_img, mask) for mask in range(2, n_p, 2)]
        other_core = [swap(block, 1) for block in same_core]
        img_blocks = [own_img, other_core[0]] + same_core[1:] + other_core[1:]
        img_all = None
        for index, block in enumerate(img_blocks):
            img_all = prep_block(block, w_img, index, n_p, img_all, True)
        held = lax.optimization_barrier((*txt_blocks[1:], img_all[1]))
        txt_blocks = [own_txt, *held[:-1]]
        img_all = (img_all[0], held[-1], *img_all[2:])
        ids_txt = jnp.concatenate([read_ids(block) for block in txt_blocks])
        ids_img = jnp.concatenate([read_ids(block) for block in img_blocks])
        id_rows = jnp.broadcast_to(ids_txt[:, None], (ids_txt.shape[0], LANES))
        id_cols = jnp.broadcast_to(ids_img[None, :], (8, ids_img.shape[0]))

        txt_all = None
        for index, block in enumerate(txt_blocks):
            txt_all = prep_block(block, w_txt, index, n_z, txt_all, False)
        emb_txt, emb_txt_t, raw_txt, x_txt = txt_all
        emb_img, emb_img_t, raw_img_t, x_img = img_all
        scal = jnp.stack([temp_scale * LOG2E, logit_bias * LOG2E])
        part_txt, part_img_t, sums = pair_call(scal, emb_txt, emb_txt_t, emb_img, emb_img_t, id_rows, id_cols)
        dw_txt_t = tail_call(part_txt, raw_txt, x_txt, False)
        dw_img_t = tail_call(part_img_t, raw_img_t, x_img, True)
        sums = jnp.sum(sums, axis=(1, 2)) / total_rows
        sums = jnp.broadcast_to(jnp.pad(sums, (0, dw_txt_t.shape[0] - 3))[:, None], (dw_txt_t.shape[0], LANES))
        total = sum_over_devices(jnp.concatenate([dw_img_t, dw_txt_t, sums], axis=1), n_z, n_p)
        scale = temp_scale / total_rows
        n_img = dw_img_t.shape[1]
        n_both = n_img + dw_txt_t.shape[1]
        sums = total[:3, n_both]
        return (sums[0], temp_scale * sums[1], sums[2],
                scale * total[:, :n_img].T, scale * total[:, n_img:n_both].T)

    return jax.shard_map(
        local_fn,
        mesh=grid_mesh,
        in_specs=(P(("z", "p"), None), P(("z", "p"), None), P(None, None), P(None, None), P(), P(), P(("z", "p"))),
        out_specs=(P(), P(), P(), P(None, None), P(None, None)),
        check_vma=False,
    )
```
